32 devices in a mesh: dp: 8 (over z, y), tensor: 4 (over x, core).
Axes of the slice: x: 2, y: 2, z: 4, core: 2. Of those that a mesh axis runs over, the one named last changes fastest.
Arguments:
- cotangent: bfloat16 [2048, 8192], P(('dp', 'tensor')), may hold values from -1.1048543 to 1.1048543
- gate_pre: bfloat16 [2048, 14336], P('dp', 'tensor'), may hold values from -5 to 5
- up_pre: bfloat16 [2048, 14336], P('dp', 'tensor'), may hold values from -28 to 28
- row_state: float32 [8192], P('dp'), may hold values from 0.02 to 3
- column_state: float32 [14336], P('tensor'), may hold values from 0.05 to 2
Outputs:
- update: float32 [8192, 14336], P('dp', 'tensor')
- row_next: float32 [8192], P('dp')
- column_next: float32 [14336], P('tensor')
- row_scale: float32 [1], replicated
The draws below stay inside these ranges and needn't reach their ends.
All inputs are finite; a program needn't handle non-finite values.
Results may differ from the reference program's by a relative error of at most 0.019.
Values may be sent and summed in bfloat16 or wider, within the bound.
A program may use at most 192 MiB of HBM per device.

```python
import math
import jax
import jax.numpy as jnp
from jax import lax

D = 8192
FF = 14336
TOK_DP = 256
TOKENS = 2048
N_DP = 8


def draw_cotangent(key, part):
    first_key, second_key = jax.random.split(key, 2)
    position = jnp.arange(D, dtype=jnp.float32) / D
    base = jnp.clip(jax.random.normal(first_key, (TOKENS, D), jnp.float32), -5.0, 5.0)
    spread = 10.0 ** (jax.random.uniform(second_key, (D,), jnp.float32) - 0.5)
    scale = spread * 3.0 ** (position - 0.5) / math.sqrt(TOKENS)
    return (base * scale[None, :]).astype(jnp.bfloat16)


def draw_up_pre(key, part):
    first_key, second_key = jax.random.split(key, 2)
    position = jnp.arange(FF, dtype=jnp.float32) / FF
    base = jnp.clip(jax.random.normal(first_key, (TOKENS, FF), jnp.float32), -5.0, 5.0)
    spread = 10.0 ** (jax.random.uniform(second_key, (FF,), jnp.float32) - 0.5)
    scale = spread * 3.0 ** (position - 0.5)
    return (base * scale[None, :]).astype(jnp.bfloat16)


def draw_row_state(key, part):
    position = jnp.arange(D, dtype=jnp.float32) / D
    level = jax.random.uniform(key, (D,), jnp.float32, 0.0, 1.0)
    return 0.02 * 10.0 ** (0.7 * level + 0.65 * position)


def shard_levels(key, shape, cuts, smallest, high):
    gain, own = 1.0, jax.random.fold_in(key, 6)
    for dim, parts in cuts:
        draws = jnp.exp(jax.random.uniform(jax.random.fold_in(own, dim), (parts,), jnp.float32, smallest / len(cuts), high / len(cuts)))
        gain = gain * jnp.repeat(draws, shape[dim] // parts).reshape([-1 if axis == dim else 1 for axis in range(len(shape))])
    return gain


def noise(stream_key, extent, width, most, cuts=(), kind=jnp.bfloat16):
    values = jax.random.normal(stream_key, extent, jnp.float32) * width
    if len(cuts) > 0:
        values = shard_levels(stream_key, extent, cuts, -0.22, 0.18) * values
    return jnp.clip(values, min=-most, max=most).astype(kind)


def setup_inputs(seed: int = 0) -> dict:
    keys = jax.random.split(jax.random.key(seed), 6)
    cotangent = draw_cotangent(jax.random.fold_in(keys[5], 71), 0)
    gate_pre = noise(keys[1], (TOKENS, FF), 1.0, 5.0, ((0, 8), (1, 4)))
    up_pre = draw_up_pre(jax.random.fold_in(keys[5], 71), 0)
    row_state = draw_row_state(jax.random.fold_in(keys[5], 71), 0)
    column_state = jnp.clip(jnp.exp(math.log(2.0) - 3.6888794 * jax.random.uniform(keys[4], (FF,), jnp.float32) ** shard_levels(keys[4], (FF,), ((0, 4),), -0.2, 0.2)), 0.05, 2.0)
    return {"cotangent": cotangent, "gate_pre": gate_pre, "up_pre": up_pre, "row_state": row_state, "column_state": column_state}


EPSILON = 1e-30
DECAY_RATE = 0.9

def reference(cotangent, gate_pre, up_pre, row_state, column_state):
    hidden = (jax.nn.silu(gate_pre.astype(jnp.float32)) * up_pre.astype(jnp.float32)).astype(jnp.bfloat16)
    cot_groups = cotangent.reshape(N_DP, TOK_DP, D)
    hid_groups = hidden.reshape(N_DP, TOK_DP, FF)

    def add_group(running, paired):
        partial_value = jnp.dot(paired[0].T, paired[1], preferred_element_type=jnp.float32)
        rounded = lax.optimization_barrier(partial_value.astype(jnp.bfloat16))
        return (running + rounded.astype(jnp.float32), None)
    gradient, _ = lax.scan(add_group, jnp.zeros((D, FF), jnp.float32), (cot_groups, hid_groups))
    squares = gradient * gradient + EPSILON
    row_next = DECAY_RATE * row_state + (1.0 - DECAY_RATE) * lax.optimization_barrier(jnp.mean(squares, axis=1))
    column_next = DECAY_RATE * column_state + (1.0 - DECAY_RATE) * lax.optimization_barrier(jnp.mean(squares, axis=0))
    row_mean = jnp.mean(row_next)
    second_moment = row_next[:, None] * column_next[None, :] / row_mean
    raw_update = gradient / jnp.sqrt(second_moment)
    norm_value = jnp.sqrt(jnp.mean(raw_update * raw_update))
    update = raw_update / jnp.maximum(1.0, norm_value)
    return (update, row_next, column_next, jnp.reshape(row_mean, (1,)))
```

```python
import functools

import jax
import jax.numpy as jnp
from jax import lax
from jax.experimental import pallas as pl
from jax.experimental.pallas import tpu as pltpu
from jax.sharding import PartitionSpec as P

EPSILON = 1e-30
DECAY_RATE = 0.9
MESH = pl.DeviceIdType.MESH
PAIR = 2
LAG = 2


def chunk_count(width):
    for count in (7, 8, 6, 5, 4, 3, 2):
        if width % (count * 128) == 0:
            return count
    return 1


def kernel(
    n_dp, n_t, chunks, rows_all, cols_all,
    cot, gate, up, row_state, column_state,
    g_out, row_out, col_out, rfac_out, cfac_out, mean_out,
    hid, cr, cot_t, grad, row_part, col_part, rbuf, cbuf, pbuf, qbuf,
    own_sem, a2a_s, a2a_r, ag_s, ag_r, hs, hr, g_sem, rs, rr, cs, cr_sem, ps, pr, qs, qr,
):
    me = lax.axis_index("dp")
    tt = lax.axis_index("tensor")
    line = n_dp // PAIR
    i = me // PAIR
    j = me % PAIR
    other = i * PAIR + (1 - j)
    width = cr.shape[3]
    tokens = hid.shape[2]
    fc = hid.shape[3]

    barrier = pltpu.get_barrier_semaphore()
    for off in range(1, n_dp):
        pl.semaphore_signal(barrier, inc=1, device_id=((me + off) % n_dp, tt), device_id_type=MESH)
    for off in range(1, n_t):
        pl.semaphore_signal(barrier, inc=1, device_id=(me, (tt + off) % n_t), device_id_type=MESH)
    pl.semaphore_wait(barrier, n_dp + n_t - 2)

    def a2a(off):
        d = (me + off) % n_dp
        return pltpu.make_async_remote_copy(
            cot.at[:, pl.ds(pl.multiple_of(d * width, width), width)],
            cr.at[me, tt], a2a_s.at[d], a2a_r.at[me],
            device_id=(d, tt), device_id_type=MESH)

    def a2a_in(off):
        g = (me + off) % n_dp
        return pltpu.make_async_remote_copy(
            cr.at[g, tt], cr.at[g, tt], a2a_s.at[g], a2a_r.at[g],
            device_id=(g, tt), device_id_type=MESH)

    def gather(off):
        t = (tt + off) % n_t
        return pltpu.make_async_remote_copy(
            cr.at[:, tt], cr.at[:, tt], ag_s.at[t], ag_r.at[tt],
            device_id=(me, t), device_id_type=MESH)

    def gather_in(off):
        t = (tt + off) % n_t
        return pltpu.make_async_remote_copy(
            cr.at[:, t], cr.at[:, t], ag_s.at[t], ag_r.at[t],
            device_id=(me, t), device_id_type=MESH)

    def move(way, c, g):
        to = (me - PAIR, me + PAIR, other)[way]
        return pltpu.make_async_remote_copy(
            hid.at[c, g], hid.at[c, g], hs.at[way, c, g], hr.at[c, g],
            device_id=(to, tt), device_id_type=MESH)

    def send_left(c, g):
        @pl.when(i > 0)
        def _():
            move(0, c, g).start()

    def send_right(c, g):
        @pl.when(i < line - 1)
        def _():
            move(1, c, g).start()

    def arrived(c, g):
        move(2, c, g).wait_recv()

    own = pltpu.make_async_copy(
        cot.at[:, pl.ds(pl.multiple_of(me * width, width), width)], cr.at[me, tt], own_sem)
    own.start()
    for off in range(1, n_dp):
        a2a(off).start()

    for c in range(chunks):
        v = gate[:, c * fc:(c + 1) * fc].astype(jnp.float32)
        u = up[:, c * fc:(c + 1) * fc].astype(jnp.float32)
        hid[c, me] = (v / (1.0 + jnp.exp(-v)) * u).astype(jnp.bfloat16)
    own.wait()

    move(2, 0, me).start()

    @pl.loop(1, chunks)
    def _(c):
        send_left(c, me)
        send_right(c, me)
        move(2, c, me).start()

    send_left(0, me)
    send_right(0, me)

    row_part[...] = jnp.zeros_like(row_part)
    col_part[...] = jnp.zeros_like(col_part)

    for off in range(1, n_dp):
        a2a_in(off).wait_recv()
    for off in range(1, n_t):
        gather(off).start()

    arrived(0, other)
    send_left(0, other)
    send_right(0, other)

    def turn(g):
        block = cr[g].reshape(tokens, width)
        cot_t[:, pl.ds(pl.multiple_of(g * tokens, 128), tokens)] = block.T

    tile = min(256, width)

    def product(c):
        @pl.loop(0, n_dp)
        def _(g):
            @pl.when((g % PAIR != j) & (c > 0))
            def _():
                arrived(c, g)

        @pl.loop(0, width // tile)
        def _(m):
            at = pl.ds(pl.multiple_of(m * tile, tile), tile)
            value = jnp.dot(cot_t[at, :], hid[c].reshape(n_dp * tokens, fc),
                            preferred_element_type=jnp.float32)
            grad[c, at, :] = value
            square = value * value + EPSILON
            col_part[c] += jnp.sum(square.reshape(tile // 8, 8, fc), axis=0)
            lanes = square[:, 0:128]
            for k in range(1, fc // 128):
                lanes = lanes + square[:, k * 128:(k + 1) * 128]
            row_part[at, :] += lanes

    def put(c):
        return pltpu.make_async_copy(grad.at[c], g_out.at[:, c * fc:(c + 1) * fc], g_sem.at[c])

    turn_hop = max(1, line - 2)
    per = -(-n_dp // max(1, chunks - 1))
    for h in range(1, line):
        last = h == line - 1
        gl = me - h * PAIR
        gr = me + h * PAIR

        def step(c, h=h, gl=gl, gr=gr):
            @pl.when(i >= h)
            def _():
                arrived(c, gl)
                send_right(c, gl)
                move(2, c, gl).start()

            @pl.when(i + h < line)
            def _():
                arrived(c, gr)
                send_left(c, gr)
                move(2, c, gr).start()

        for c in range(1, chunks):
            step(c)
            if h == turn_hop:
                if c == 1:
                    for off in range(1, n_t):
                        gather_in(off).wait_recv()
                for g in range((c - 1) * per, min(c * per, n_dp)):
                    turn(g)
            if last and c - LAG >= 1:
                product(c - LAG)
        for jj in (j, 1 - j):
            ql = (i - h) * PAIR + jj
            qr_ = (i + h) * PAIR + jj

            @pl.when(i >= h)
            def _():
                arrived(0, ql)
                send_right(0, ql)

            @pl.when(i + h < line)
            def _():
                arrived(0, qr_)
                send_left(0, qr_)

    if chunks == 1:
        for off in range(1, n_t):
            gather_in(off).wait_recv()
        for g in range(n_dp):
            turn(g)
    for c in range(max(1, chunks - LAG), chunks):
        product(c)
    product(0)

    rbuf[tt] = jnp.sum(row_part[...].T, axis=0, keepdims=True)
    for c in range(chunks):
        cbuf[me, c] = jnp.sum(col_part[c], axis=0, keepdims=True)

    def rmove(off, mine):
        t = (tt + off) % n_t
        k = tt if mine else t
        return pltpu.make_async_remote_copy(
            rbuf.at[k], rbuf.at[k], rs.at[t], rr.at[k], device_id=(me, t), device_id_type=MESH)

    def cmove(off, mine):
        d = (me + off) % n_dp
        k = me if mine else d
        return pltpu.make_async_remote_copy(
            cbuf.at[k], cbuf.at[k], cs.at[d], cr_sem.at[k], device_id=(d, tt), device_id_type=MESH)

    def pmove(off, mine):
        t = (tt + off) % n_t
        k = tt if mine else t
        return pltpu.make_async_remote_copy(
            pbuf.at[k], pbuf.at[k], ps.at[t], pr.at[k], device_id=(me, t), device_id_type=MESH)

    def qmove(off, mine):
        d = (me + off) % n_dp
        k = me if mine else d
        return pltpu.make_async_remote_copy(
            qbuf.at[k], qbuf.at[k], qs.at[d], qr.at[k], device_id=(d, tt), device_id_type=MESH)

    for off in range(1, n_dp):
        cmove(off, True).start()
    for off in range(1, n_t):
        rmove(off, True).start()
    for c in range(chunks):
        put(c).start()

    @pl.loop(0, chunks)
    def _(c):
        @pl.loop(0, n_dp)
        def _(g):
            gi = g // PAIR
            mine = g % PAIR == j

            @pl.when((i > 0) & (gi >= i) & (mine | (c == 0)))
            def _():
                move(0, c, g).wait_send()

            @pl.when((i < line - 1) & (gi <= i) & (mine | (c == 0)))
            def _():
                move(1, c, g).wait_send()

            @pl.when(mine & ((gi == i) | (c > 0)))
            def _():
                move(2, c, g).wait_send()

    for off in range(1, n_dp):
        a2a(off).wait_send()
    for off in range(1, n_t):
        gather(off).wait_send()

    for off in range(1, n_t):
        rmove(off, False).wait_recv()
    row_total = rbuf[0]
    for t in range(1, n_t):
        row_total = row_total + rbuf[t]
    row_next = DECAY_RATE * row_state[...] + (1.0 - DECAY_RATE) * (row_total / cols_all)
    row_out[...] = row_next
    weight = 1.0 / row_next
    row_part[...] = jnp.broadcast_to(weight, (128, width)).T

    for off in range(1, n_dp):
        cmove(off, False).wait_recv()
    total = jnp.zeros((8, fc), jnp.float32)
    for c in range(chunks):
        col_total = cbuf[0, c]
        for d in range(1, n_dp):
            col_total = col_total + cbuf[d, c]
        col_next = DECAY_RATE * column_state[c] + (1.0 - DECAY_RATE) * (col_total / rows_all)
        col_out[c] = col_next

        def body(m, carry, c=c):
            at = pl.ds(pl.multiple_of(m * tile, tile), tile)
            w = row_part[at, :]
            parts = []
            for k in range(fc // 128):
                value = grad[c, at, k * 128:(k + 1) * 128]
                parts.append(jnp.sum((value * value * w).reshape(tile // 8, 8, 128), axis=0))
            return carry + jnp.concatenate(parts, axis=1)

        weighted = lax.fori_loop(0, width // tile, body, jnp.zeros((8, fc), jnp.float32))
        total = total + weighted * (1.0 / col_next)

    def whole_sum(x):
        return jnp.sum(jnp.sum(x, axis=1, keepdims=True), axis=0, keepdims=True)

    pbuf[tt] = jnp.broadcast_to(whole_sum(total), (8, 128))
    for off in range(1, n_t):
        pmove(off, True).start()
    row_sum = whole_sum(row_next)
    for off in range(1, n_t):
        pmove(off, False).wait_recv()
    square_sum = pbuf[0]
    for t in range(1, n_t):
        square_sum = square_sum + pbuf[t]
    qbuf[me, 0:8] = square_sum
    qbuf[me, 8:16] = jnp.broadcast_to(row_sum, (8, 128))
    for off in range(1, n_dp):
        qmove(off, True).start()
    for off in range(1, n_dp):
        qmove(off, False).wait_recv()
    sums = qbuf[0]
    for d in range(1, n_dp):
        sums = sums + qbuf[d]
    mean = sums[8:9, 0:1] / rows_all
    norm = jnp.sqrt(mean * (sums[0:1, 0:1] / rows_all / cols_all))
    factor = jnp.sqrt(mean) / jnp.maximum(1.0, norm)
    mean_out[...] = jnp.broadcast_to(mean, (1, 128))
    rfac_out[...] = factor * lax.rsqrt(row_next)
    for c in range(chunks):
        cfac_out[c] = lax.rsqrt(col_out[c])

    for off in range(1, n_dp):
        cmove(off, True).wait_send()
        qmove(off, True).wait_send()
    for off in range(1, n_t):
        rmove(off, True).wait_send()
        pmove(off, True).wait_send()
    for c in range(chunks):
        put(c).wait()


def solution(mesh):
    n_dp, n_t = mesh.shape["dp"], mesh.shape["tensor"]

    def shards(cotangent, gate_pre, up_pre, row_state, column_state):
        rows_each, d_all = cotangent.shape
        tokens, ff = gate_pre.shape
        width = row_state.shape[0]
        chunks = chunk_count(ff)
        fc = ff // chunks
        f32, bf16 = jnp.float32, jnp.bfloat16
        dma, vmem = pltpu.SemaphoreType.DMA, pltpu.VMEM
        spec = pl.BlockSpec(memory_space=pltpu.VMEM)
        grad, row_next, col_next, rfac, cfac, mean = pl.pallas_call(
            functools.partial(kernel, n_dp, n_t, chunks, float(d_all), float(ff * n_t)),
            out_shape=(
                jax.ShapeDtypeStruct((width, ff), f32),
                jax.ShapeDtypeStruct((1, width), f32),
                jax.ShapeDtypeStruct((chunks, 1, fc), f32),
                jax.ShapeDtypeStruct((1, width), f32),
                jax.ShapeDtypeStruct((chunks, 1, fc), f32),
                jax.ShapeDtypeStruct((1, 128), f32),
            ),
            in_specs=[spec] * 5,
            out_specs=(pl.BlockSpec(memory_space=pl.ANY),) + (spec,) * 5,
            scratch_shapes=[
                vmem((chunks, n_dp, tokens, fc), bf16),
                vmem((n_dp, n_t, rows_each, width), bf16),
                vmem((width, n_dp * tokens), bf16),
                vmem((chunks, width, fc), f32),
                vmem((width, 128), f32),
                vmem((chunks, 8, fc), f32),
                vmem((n_t, 1, width), f32),
                vmem((n_dp, chunks, 1, fc), f32),
                vmem((n_t, 8, 128), f32),
                vmem((n_dp, 16, 128), f32),
                dma, dma((n_dp,)), dma((n_dp,)), dma((n_t,)), dma((n_t,)),
                dma((3, chunks, n_dp)), dma((chunks, n_dp)), dma((chunks,)),
                dma((n_t,)), dma((n_t,)), dma((n_dp,)), dma((n_dp,)),
                dma((n_t,)), dma((n_t,)), dma((n_dp,)), dma((n_dp,)),
            ],
            compiler_params=pltpu.CompilerParams(
                collective_id=0, has_side_effects=True, vmem_limit_bytes=60 * 1024 * 1024),
        )(cotangent, gate_pre, up_pre, row_state.reshape(1, width),
          column_state.reshape(chunks, 1, fc))
        update = grad * rfac.reshape(width)[:, None] * cfac.reshape(ff)[None, :]
        return (update, row_next.reshape(width), col_next.reshape(ff), mean[0, 0:1])

    return jax.shard_map(
        shards,
        mesh=mesh,
        in_specs=(
            P(("dp", "tensor"), None),
            P("dp", "tensor"),
            P("dp", "tensor"),
            P("dp"),
            P("tensor"),
        ),
        out_specs=(P("dp", "tensor"), P("dp"), P("tensor"), P()),
        check_vma=False,
    )
```

```python
import functools

import jax
import jax.numpy as jnp
from jax import lax
from jax.experimental import pallas as pl
from jax.experimental.pallas import tpu as pltpu
from jax.sharding import PartitionSpec as P

EPSILON = 1e-30
DECAY_RATE = 0.9
MESH = pl.DeviceIdType.MESH
PAIR = 2
LAG = 2
GRANT = 46


def chunk_count(width):
    for count in (7, 8, 6, 5, 4, 3, 2):
        if width % (count * 128) == 0:
            return count
    return 1


def kernel(
    n_dp, n_t, chunks, rows_all, cols_all,
    cot, gate_in, up_in, row_state, column_state,
    grad, row_out, col_out, rfac_out, cfac_out, mean_out,
    gate, up, hid, cr, cot_t, row_part, col_part, rbuf, cbuf, pbuf, qbuf,
    own_sem, load_sem, a2a_s, a2a_r, ag_s, ag_r, hs, hr, rs, rr, cs, cr_sem, ps, pr, qs, qr,
):
    me = lax.axis_index("dp")
    tt = lax.axis_index("tensor")
    line = n_dp // PAIR
    i = me // PAIR
    j = me % PAIR
    other = i * PAIR + (1 - j)
    width = cr.shape[3]
    tokens = hid.shape[2]
    fc = hid.shape[3]

    loads = [pltpu.make_async_copy(gate_in, gate, load_sem.at[0]),
             pltpu.make_async_copy(up_in, up, load_sem.at[1])]
    for load in loads:
        load.start()

    barrier = pltpu.get_barrier_semaphore()
    for off in range(1, n_dp):
        pl.semaphore_signal(barrier, inc=1, device_id=((me + off) % n_dp, tt), device_id_type=MESH)
    for off in range(1, n_t):
        pl.semaphore_signal(barrier, inc=1, device_id=(me, (tt + off) % n_t), device_id_type=MESH)
    pl.semaphore_wait(barrier, n_dp + n_t - 2)

    def a2a(off):
        d = (me + off) % n_dp
        return pltpu.make_async_remote_copy(
            cot.at[:, pl.ds(pl.multiple_of(d * width, width), width)],
            cr.at[me, tt], a2a_s.at[d], a2a_r.at[me],
            device_id=(d, tt), device_id_type=MESH)

    def a2a_in(off):
        g = (me + off) % n_dp
        return pltpu.make_async_remote_copy(
            cr.at[g, tt], cr.at[g, tt], a2a_s.at[g], a2a_r.at[g],
            device_id=(g, tt), device_id_type=MESH)

    def gather(off):
        t = (tt + off) % n_t
        return pltpu.make_async_remote_copy(
            cr.at[:, tt], cr.at[:, tt], ag_s.at[t], ag_r.at[tt],
            device_id=(me, t), device_id_type=MESH)

    def gather_in(off):
        t = (tt + off) % n_t
        return pltpu.make_async_remote_copy(
            cr.at[:, t], cr.at[:, t], ag_s.at[t], ag_r.at[t],
            device_id=(me, t), device_id_type=MESH)

    def move(way, c, g):
        to = (me - PAIR, me + PAIR, other)[way]
        return pltpu.make_async_remote_copy(
            hid.at[c, g], hid.at[c, g], hs.at[way, c, g], hr.at[c, g],
            device_id=(to, tt), device_id_type=MESH)

    def send_left(c, g):
        @pl.when(i > 0)
        def _():
            move(0, c, g).start()

    def send_right(c, g):
        @pl.when(i < line - 1)
        def _():
            move(1, c, g).start()

    def arrived(c, g):
        move(2, c, g).wait_recv()

    own = pltpu.make_async_copy(
        cot.at[:, pl.ds(pl.multiple_of(me * width, width), width)], cr.at[me, tt], own_sem)
    own.start()
    for off in range(1, n_dp):
        a2a(off).start()

    for load in loads:
        load.wait()
    for c in range(chunks):
        v = gate[:, c * fc:(c + 1) * fc].astype(jnp.float32)
        u = up[:, c * fc:(c + 1) * fc].astype(jnp.float32)
        hid[c, me] = (v / (1.0 + jnp.exp(-v)) * u).astype(jnp.bfloat16)
    own.wait()

    move(2, 0, me).start()

    @pl.loop(1, chunks)
    def _(c):
        send_left(c, me)
        send_right(c, me)
        move(2, c, me).start()

    send_left(0, me)
    send_right(0, me)

    row_part[...] = jnp.zeros_like(row_part)
    col_part[...] = jnp.zeros_like(col_part)

    for off in range(1, n_dp):
        a2a_in(off).wait_recv()
    for off in range(1, n_t):
        gather(off).start()

    arrived(0, other)
    send_left(0, other)
    send_right(0, other)

    def turn(g):
        block = cr[g].reshape(tokens, width)
        cot_t[:, pl.ds(pl.multiple_of(g * tokens, 128), tokens)] = block.T

    tile = min(256, width)

    late = min(PAIR, n_dp)
    early = n_dp - late
    low = (i < (line + 1) // 2).astype(jnp.int32)
    early_at = (1 - low) * late
    late_at = low * early

    def multiply(c, first, count, fresh, final):
        cols = slice(c * fc, (c + 1) * fc)
        depth = pl.ds(pl.multiple_of(first * tokens, 128), count * tokens)

        @pl.loop(0, width // tile)
        def _(m):
            at = pl.ds(pl.multiple_of(m * tile, tile), tile)
            value = jnp.dot(cot_t[at, depth], hid[c, pl.ds(first, count)].reshape(count * tokens, fc),
                            preferred_element_type=jnp.float32)
            if not fresh:
                value = value + grad[at, cols]
            grad[at, cols] = value
            if final:
                square = value * value + EPSILON
                col_part[c] += jnp.sum(square.reshape(tile // 8, 8, fc), axis=0)
                lanes = square[:, 0:128]
                for k in range(1, fc // 128):
                    lanes = lanes + square[:, k * 128:(k + 1) * 128]
                row_part[at, :] += lanes

    def crossed(c, first, count):
        if c > 0:
            for k in range(count // PAIR):
                arrived(c, first + k * PAIR + (1 - j))

    def product_early(c):
        if early:
            crossed(c, early_at, early)
            multiply(c, early_at, early, True, False)

    def collect(c):
        @pl.loop(0, n_dp)
        def _(g):
            gi = g // PAIR
            mine = g % PAIR == j
            z_line = mine if c > 0 else g >= 0

            @pl.when((i > 0) & (gi >= i) & z_line)
            def _():
                move(0, c, g).wait_send()

            @pl.when((i < line - 1) & (gi <= i) & z_line)
            def _():
                move(1, c, g).wait_send()

            @pl.when(mine if c > 0 else mine & (gi == i))
            def _():
                move(2, c, g).wait_send()

    def product_late(c):
        crossed(c, late_at, late)
        multiply(c, late_at, late, not early, True)

    turn_hop = max(1, line - 2)
    skip = (chunks - 1) // 2
    per = -(-n_dp // max(1, chunks - 1 - skip))
    for h in range(1, line):
        last = h == line - 1
        gl = me - h * PAIR
        gr = me + h * PAIR

        def step(c, h=h, gl=gl, gr=gr):
            @pl.when(i >= h)
            def _():
                arrived(c, gl)
                send_right(c, gl)
                move(2, c, gl).start()

            @pl.when(i + h < line)
            def _():
                arrived(c, gr)
                send_left(c, gr)
                move(2, c, gr).start()

        for c in range(1, chunks):
            step(c)
            if h == turn_hop and c > skip:
                if c == skip + 1:
                    for off in range(1, n_t):
                        gather_in(off).wait_recv()
                for g in range((c - 1 - skip) * per, min((c - skip) * per, n_dp)):
                    turn(g)
            if last:
                if c == 1:
                    product_early(1)
                    product_early(2 % chunks)
                elif c + 1 < chunks:
                    product_early(c + 1)
                else:
                    product_early(0)
                if c - LAG >= 1:
                    product_late(c - LAG)
                    collect(c - LAG)
        for jj in (j, 1 - j):
            ql = (i - h) * PAIR + jj
            qr_ = (i + h) * PAIR + jj

            @pl.when(i >= h)
            def _():
                arrived(0, ql)
                send_right(0, ql)

            @pl.when(i + h < line)
            def _():
                arrived(0, qr_)
                send_left(0, qr_)

    for c in range(chunks - LAG, chunks):
        product_late(c)
    product_late(0)

    rbuf[tt] = jnp.sum(row_part[...].T, axis=0, keepdims=True)
    for c in range(chunks):
        cbuf[me, c] = jnp.sum(col_part[c], axis=0, keepdims=True)

    def rmove(off, mine):
        t = (tt + off) % n_t
        k = tt if mine else t
        return pltpu.make_async_remote_copy(
            rbuf.at[k], rbuf.at[k], rs.at[t], rr.at[k], device_id=(me, t), device_id_type=MESH)

    def cmove(off, mine):
        d = (me + off) % n_dp
        k = me if mine else d
        return pltpu.make_async_remote_copy(
            cbuf.at[k], cbuf.at[k], cs.at[d], cr_sem.at[k], device_id=(d, tt), device_id_type=MESH)

    def pmove(off, mine):
        t = (tt + off) % n_t
        k = tt if mine else t
        return pltpu.make_async_remote_copy(
            pbuf.at[k], pbuf.at[k], ps.at[t], pr.at[k], device_id=(me, t), device_id_type=MESH)

    def qmove(off, mine):
        d = (me + off) % n_dp
        k = me if mine else d
        return pltpu.make_async_remote_copy(
            qbuf.at[k], qbuf.at[k], qs.at[d], qr.at[k], device_id=(d, tt), device_id_type=MESH)

    for off in range(1, n_dp):
        cmove(off, True).start()
    for off in range(1, n_t):
        rmove(off, True).start()

    for c in (0,) + tuple(range(max(1, chunks - LAG), chunks)):
        collect(c)
    for off in range(1, n_dp):
        a2a(off).wait_send()
    for off in range(1, n_t):
        gather(off).wait_send()

    for off in range(1, n_t):
        rmove(off, False).wait_recv()
    row_total = rbuf[0]
    for t in range(1, n_t):
        row_total = row_total + rbuf[t]
    row_next = DECAY_RATE * row_state[...] + (1.0 - DECAY_RATE) * (row_total / cols_all)
    row_out[...] = row_next
    weight = 1.0 / row_next
    row_part[...] = jnp.broadcast_to(weight, (128, width)).T
    rfac_out[...] = jnp.sqrt(row_part[...])

    for c in range(chunks):
        def body(m, carry, c=c):
            at = pl.ds(pl.multiple_of(m * tile, tile), tile)
            w = row_part[at, :]
            parts = []
            for k in range(fc // 128):
                value = grad[at, c * fc + k * 128:c * fc + (k + 1) * 128]
                parts.append(jnp.sum((value * value * w).reshape(tile // 8, 8, 128), axis=0))
            return carry + jnp.concatenate(parts, axis=1)

        col_part[c] = lax.fori_loop(0, width // tile, body, jnp.zeros((8, fc), jnp.float32))

    for off in range(1, n_dp):
        cmove(off, False).wait_recv()
    total = jnp.zeros((8, fc), jnp.float32)
    for c in range(chunks):
        col_total = cbuf[0, c]
        for d in range(1, n_dp):
            col_total = col_total + cbuf[d, c]
        col_next = DECAY_RATE * column_state[:, c * fc:(c + 1) * fc] + (1.0 - DECAY_RATE) * (col_total / rows_all)
        col_out[:, c * fc:(c + 1) * fc] = col_next
        total = total + col_part[c] * (1.0 / col_next)

    def whole_sum(x):
        return jnp.sum(jnp.sum(x, axis=1, keepdims=True), axis=0, keepdims=True)

    pbuf[tt] = jnp.broadcast_to(whole_sum(total), (8, 128))
    for off in range(1, n_t):
        pmove(off, True).start()
    row_sum = whole_sum(row_next)
    for off in range(1, n_t):
        pmove(off, False).wait_recv()
    square_sum = pbuf[0]
    for t in range(1, n_t):
        square_sum = square_sum + pbuf[t]
    qbuf[me, 0:8] = square_sum
    qbuf[me, 8:16] = jnp.broadcast_to(row_sum, (8, 128))
    for off in range(1, n_dp):
        qmove(off, True).start()
    for off in range(1, n_dp):
        qmove(off, False).wait_recv()
    sums = qbuf[0]
    for d in range(1, n_dp):
        sums = sums + qbuf[d]
    mean = sums[8:9, 0:1] / rows_all
    norm = jnp.sqrt(mean * (sums[0:1, 0:1] / rows_all / cols_all))
    factor = jnp.sqrt(mean) / jnp.maximum(1.0, norm)
    mean_out[...] = jnp.broadcast_to(mean, (1, 128))
    cfac_out[...] = factor * lax.rsqrt(col_out[...])

    for off in range(1, n_dp):
        cmove(off, True).wait_send()
        qmove(off, True).wait_send()
    for off in range(1, n_t):
        rmove(off, True).wait_send()
        pmove(off, True).wait_send()


def scale(rows, grad, rfac, cfac, out):
    at = pl.ds(pl.multiple_of(pl.program_id(0) * rows, rows), rows)
    row = rfac[at, :]
    for k in range(grad.shape[1] // 128):
        cols = slice(k * 128, (k + 1) * 128)
        out[:, cols] = grad[at, cols] * row * cfac[:, cols]


def solution(mesh):
    n_dp, n_t = mesh.shape["dp"], mesh.shape["tensor"]

    def shards(cotangent, gate_pre, up_pre, row_state, column_state):
        rows_each, d_all = cotangent.shape
        tokens, ff = gate_pre.shape
        width = row_state.shape[0]
        chunks = chunk_count(ff)
        fc = ff // chunks
        f32, bf16 = jnp.float32, jnp.bfloat16
        dma, vmem = pltpu.SemaphoreType.DMA, pltpu.VMEM
        spec = pl.BlockSpec(memory_space=pltpu.VMEM)
        grad, row_next, col_next, rfac, cfac, mean = pl.pallas_call(
            functools.partial(kernel, n_dp, n_t, chunks, float(d_all), float(ff * n_t)),
            out_shape=(
                pltpu.VMEM((width, ff), f32),
                jax.ShapeDtypeStruct((1, width), f32),
                jax.ShapeDtypeStruct((1, ff), f32),
                pltpu.VMEM((width, 128), f32),
                pltpu.VMEM((1, ff), f32),
                jax.ShapeDtypeStruct((1, 128), f32),
            ),
            in_specs=[pl.BlockSpec(memory_space=pl.ANY)] * 3 + [spec] * 2,
            out_specs=(spec,) * 6,
            scratch_shapes=[
                vmem((tokens, ff), bf16),
                vmem((tokens, ff), bf16),
                vmem((chunks, n_dp, tokens, fc), bf16),
                vmem((n_dp, n_t, rows_each, width), bf16),
                vmem((width, n_dp * tokens), bf16),
                vmem((width, 128), f32),
                vmem((chunks, 8, fc), f32),
                vmem((n_t, 1, width), f32),
                vmem((n_dp, chunks, 1, fc), f32),
                vmem((n_t, 8, 128), f32),
                vmem((n_dp, 16, 128), f32),
                dma, dma((2,)), dma((n_dp,)), dma((n_dp,)), dma((n_t,)), dma((n_t,)),
                dma((3, chunks, n_dp)), dma((chunks, n_dp)),
                dma((n_t,)), dma((n_t,)), dma((n_dp,)), dma((n_dp,)),
                dma((n_t,)), dma((n_t,)), dma((n_dp,)), dma((n_dp,)),
            ],
            compiler_params=pltpu.CompilerParams(
                collective_id=0, has_side_effects=True, vmem_limit_bytes=GRANT * 1024 * 1024),
        )(cotangent, gate_pre, up_pre, row_state.reshape(1, width),
          column_state.reshape(1, ff))
        rows = min(128, width)
        update = pl.pallas_call(
            functools.partial(scale, rows),
            out_shape=jax.ShapeDtypeStruct((width, ff), f32),
            grid=(width // rows,),
            in_specs=[spec] * 3,
            out_specs=pl.BlockSpec((rows, ff), lambda m: (m, 0)),
            compiler_params=pltpu.CompilerParams(vmem_limit_bytes=16 * 1024 * 1024),
        )(grad, rfac, cfac)
        return (update, row_next.reshape(width), col_next.reshape(ff), mean[0, 0:1])

    return jax.shard_map(
        shards,
        mesh=mesh,
        in_specs=(
            P(("dp", "tensor"), None),
            P("dp", "tensor"),
            P("dp", "tensor"),
            P("dp"),
            P("tensor"),
        ),
        out_specs=(P("dp", "tensor"), P("dp"), P("tensor"), P()),
        check_vma=False,
    )
```
